32 devices in a mesh: row: 8 (over z, x), col: 4 (over y, core).
Axes of the slice: x: 2, y: 2, z: 4, core: 2. Of those that a mesh axis runs over, the one named last changes fastest.
Arguments:
- field: bfloat16 [192, 128, 256], P('row', 'col'), may hold values from -6 to 6
- gains: float32 [1, 2, 256], replicated, may hold values from 0.5 to 1.5
- w_query: bfloat16 [1, 256, 256], replicated, may hold values from -24 to 24
- w_key: bfloat16 [1, 256, 256], replicated, may hold values from -1 to 1
- w_value: bfloat16 [1, 256, 256], replicated, may hold values from -0.375 to 0.375
- w_out: bfloat16 [1, 256, 256], replicated, may hold values from -0.375 to 0.375
- w_up: bfloat16 [1, 256, 1024], replicated, may hold values from -0.375 to 0.375
- w_down: bfloat16 [1, 1024, 256], replicated, may hold values from -0.1875 to 0.1875
- final_gain: float32 [256], replicated, may hold values from 0.5 to 1.5
- conv_weight: bfloat16 [3, 3, 256, 256], replicated, may hold values from -0.125 to 0.125
Outputs:
- image: float32 [16, 768, 512], P(None, 'row', 'col')
The draws below stay inside these ranges and needn't reach their ends.
All inputs are finite; a program needn't handle non-finite values.
Results may differ from the reference program's by a relative error of at most 0.0056.
Values may be sent and summed in bfloat16 or wider, within the bound.
A program may use at most 64 MiB of HBM per device.

```python
import jax
import jax.numpy as jnp
from jax import lax

D = 256
HEADS = 8
FF = 1024
HEAD = 32
WH = 24
WW = 32
HALO = 8
LAYERS = 1
OUT_CH = 16
SHUF = 4
ROWS = 192
COLS = 128


def query_and_key(key):
    base = jax.random.fold_in(key, 17)
    first, second = jax.random.split(base, 2)
    bound = min(3.0 * D ** (-0.5), 1.0)
    w_key = jnp.clip(jax.random.normal(first, (LAYERS, D, D), jnp.float32) * D ** (-0.5), -bound, bound)
    noise = jnp.clip(jax.random.normal(second, (LAYERS, D, D), jnp.float32) * D ** (-0.5), -bound, bound)
    w_query = noise
    return (w_query, w_key)


def draw_w_query(key, part):
    return query_and_key(key)[0].astype(jnp.bfloat16)


def draw_w_key(key, part):
    return query_and_key(key)[1].astype(jnp.bfloat16)


def shard_levels(own_key, shape, cuts, least, largest):
    level, own = 1.0, jax.random.fold_in(own_key, 6)
    for dim, blocks in cuts:
        draws = jnp.exp(jax.random.uniform(jax.random.fold_in(own, dim), (blocks,), jnp.float32, least / len(cuts), largest / len(cuts)))
        level = level * jnp.repeat(draws, shape[dim] // blocks).reshape([-1 if axis == dim else 1 for axis in range(len(shape))])
    return level


def centred(own_key, extent, deviation, most, cuts=(), held_as=jnp.bfloat16):
    values = deviation * jax.random.normal(own_key, extent, jnp.float32)
    if cuts:
        values = values * shard_levels(own_key, extent, cuts, -0.22, 0.18)
    return jnp.clip(values, -most, most).astype(held_as)


def setup_inputs(seed: int = 0) -> dict:
    splits = jax.random.split(jax.random.key(seed), 11)
    field = centred(splits[0], (ROWS, COLS, D), 1.0, 6.0, ((0, 8), (1, 4)))
    gains = jnp.clip(jax.random.uniform(splits[1], (LAYERS, 2, D), jnp.float32, 0.5, 1.5), 0.5, 1.5)
    w_query = draw_w_query(jax.random.fold_in(splits[10], 71), 0)
    w_key = draw_w_key(jax.random.fold_in(splits[10], 71), 0)
    w_value = centred(splits[4], (LAYERS, D, D), D ** -0.5, 0.375)
    w_out = centred(splits[5], (LAYERS, D, D), D ** -0.5, 0.375)
    w_up = centred(splits[6], (LAYERS, D, FF), D ** -0.5, 0.375)
    w_down = centred(splits[7], (LAYERS, FF, D), FF ** -0.5, 0.1875)
    final_gain = jnp.clip(jax.random.uniform(splits[8], (D,), jnp.float32, 0.5, 1.5), 0.5, 1.5)
    conv_weight = centred(splits[9], (3, 3, D, OUT_CH * SHUF * SHUF), (9 * D) ** -0.5, 0.125)
    return {"field": field, "gains": gains, "w_query": w_query, "w_key": w_key, "w_value": w_value, "w_out": w_out, "w_up": w_up, "w_down": w_down, "final_gain": final_gain, "conv_weight": conv_weight}


def rms(values, gain):
    return values * lax.rsqrt(lax.optimization_barrier(jnp.mean(values * values, axis=-1, keepdims=True)) + 1e-06) * gain

def attend(query, keys, values, valid):
    count = query.shape[0]
    width = keys.shape[0]
    q_heads = query.reshape(count, HEADS, HEAD).transpose(1, 0, 2)
    k_heads = keys.reshape(width, HEADS, HEAD).transpose(1, 0, 2)
    v_heads = values.reshape(width, HEADS, HEAD).transpose(1, 0, 2)

    def one_head(items):
        q_one, k_one, v_one = items
        scores = jnp.dot(q_one, k_one.T, preferred_element_type=jnp.float32) * HEAD ** (-0.5)
        scores = jnp.where(valid[None, :], scores, jnp.float32(-1e+30))
        top = lax.optimization_barrier(jnp.max(scores, axis=-1, keepdims=True))
        expo = jnp.exp(scores - top)
        weights = (expo / lax.optimization_barrier(jnp.sum(expo, axis=-1, keepdims=True))).astype(jnp.bfloat16)
        return jnp.dot(weights, v_one, preferred_element_type=jnp.float32)
    merged = lax.map(one_head, (q_heads, k_heads, v_heads))
    return merged.transpose(1, 0, 2).reshape(count, HEADS * HEAD).astype(jnp.bfloat16)

def reference(field, gains, w_query, w_key, w_value, w_out, w_up, w_down, final_gain, conv_weight):
    x = field.astype(jnp.float32)
    nrow = ROWS // WH
    ncol = COLS // WW
    pads = ((HALO, HALO), (HALO, HALO), (0, 0))
    validp = jnp.pad(jnp.ones((ROWS, COLS), jnp.float32), pads[:2]) > 0.5
    for layer in range(LAYERS):
        normed = rms(x, gains[layer, 0]).astype(jnp.bfloat16).reshape(-1, D)
        query = jnp.dot(normed, w_query[layer], preferred_element_type=jnp.float32).astype(jnp.bfloat16).reshape(ROWS, COLS, D)
        keys = jnp.dot(normed, w_key[layer], preferred_element_type=jnp.float32).astype(jnp.bfloat16).reshape(ROWS, COLS, D)
        values = jnp.dot(normed, w_value[layer], preferred_element_type=jnp.float32).astype(jnp.bfloat16).reshape(ROWS, COLS, D)
        keys_pad = jnp.pad(keys, pads)
        values_pad = jnp.pad(values, pads)

        def window(index):
            first = index // ncol * WH
            second = index % ncol * WW
            zero = jnp.zeros((), jnp.int32)
            q_block = lax.dynamic_slice(query, (first, second, zero), (WH, WW, D)).reshape(-1, D)
            k_block = lax.dynamic_slice(keys_pad, (first, second, zero), (WH + 2 * HALO, WW + 2 * HALO, D)).reshape(-1, D)
            v_block = lax.dynamic_slice(values_pad, (first, second, zero), (WH + 2 * HALO, WW + 2 * HALO, D)).reshape(-1, D)
            m_block = lax.dynamic_slice(validp, (first, second), (WH + 2 * HALO, WW + 2 * HALO)).reshape(-1)
            return attend(q_block, k_block, v_block, m_block)
        context = lax.map(window, jnp.arange(nrow * ncol, dtype=jnp.int32))
        context = context.reshape(nrow, ncol, WH, WW, D).transpose(0, 2, 1, 3, 4).reshape(-1, D)
        x = x + jnp.dot(context, w_out[layer], preferred_element_type=jnp.float32).reshape(ROWS, COLS, D)
        second_norm = rms(x, gains[layer, 1]).astype(jnp.bfloat16).reshape(-1, D)
        hidden = jax.nn.gelu(jnp.dot(second_norm, w_up[layer], preferred_element_type=jnp.float32)).astype(jnp.bfloat16)
        x = x + jnp.dot(hidden, w_down[layer], preferred_element_type=jnp.float32).reshape(ROWS, COLS, D)
    final = rms(x, final_gain).astype(jnp.bfloat16)
    padded = jnp.pad(final, ((1, 1), (1, 1), (0, 0)))
    conv = jnp.zeros((ROWS * COLS, OUT_CH * SHUF * SHUF), jnp.float32)
    for first in range(3):
        for second in range(3):
            piece = padded[first:first + ROWS, second:second + COLS].reshape(-1, D)
            conv = conv + jnp.dot(piece, conv_weight[first, second], preferred_element_type=jnp.float32)
    image = conv.reshape(ROWS, COLS, OUT_CH, SHUF, SHUF).transpose(2, 0, 3, 1, 4)
    return image.reshape(OUT_CH, ROWS * SHUF, COLS * SHUF)
```

```python
import functools

import jax
import jax.numpy as jnp
from jax import lax
from jax.experimental import pallas as pl
from jax.experimental.pallas import tpu as pltpu
from jax.sharding import PartitionSpec as P

HEADS = 8
HALO = 8
SHUF = 4
CHUNK = 128
VMEM_LIMIT = 56 * 1024 * 1024
BF = jnp.bfloat16
F32 = jnp.float32
NEIGHBOURS = ((-1, 0), (1, 0), (0, -1), (0, 1), (-1, -1), (-1, 1), (1, -1), (1, 1))


def rms(values, gain):
    return values * lax.rsqrt(jnp.mean(values * values, axis=-1, keepdims=True) + 1e-06) * gain


def there(step, sizes):
    row, col = lax.axis_index("row"), lax.axis_index("col")
    nrow, ncol = row + step[0], col + step[1]
    ok = (nrow >= 0) & (nrow < sizes[0]) & (ncol >= 0) & (ncol < sizes[1])
    return ok, nrow, ncol


def greet(sizes):
    barrier = pltpu.get_barrier_semaphore()
    for step in NEIGHBOURS:
        ok, nrow, ncol = there(step, sizes)

        @pl.when(ok)
        def _():
            pl.semaphore_signal(
                barrier, inc=1, device_id=(nrow, ncol), device_id_type=pl.DeviceIdType.MESH
            )

    peers = jnp.int32(0)
    for step in NEIGHBOURS:
        peers = peers + there(step, sizes)[0].astype(jnp.int32)
    pl.semaphore_wait(barrier, peers)


def swap(sizes, sources, slots, send, recv, fills):
    copies = []
    for n, step in enumerate(NEIGHBOURS):
        ok, nrow, ncol = there(step, sizes)
        back = NEIGHBOURS.index((-step[0], -step[1]))
        copy = pltpu.make_async_remote_copy(
            src_ref=sources[n],
            dst_ref=slots[back],
            send_sem=send.at[n],
            recv_sem=recv.at[back],
            device_id=(nrow, ncol),
            device_id_type=pl.DeviceIdType.MESH,
        )
        arrival = pltpu.make_async_remote_copy(
            src_ref=slots[n],
            dst_ref=slots[n],
            send_sem=send.at[n],
            recv_sem=recv.at[n],
            device_id=(nrow, ncol),
            device_id_type=pl.DeviceIdType.MESH,
        )
        copies.append((ok, copy, arrival))
        pl.when(ok)(copy.start)
        pl.when(jnp.logical_not(ok))(fills[n])
    return copies


def finish(copies):
    for ok, copy, arrival in copies:
        pl.when(ok)(arrival.wait_recv)
    for ok, copy, _ in copies:
        pl.when(ok)(copy.wait_send)


def pieces(rows, groups):
    return [HALO * groups] * 2 + [rows] * 2 + [HALO] * 4


def halo_kernel(sizes, field_ref, halo_ref, send, recv):
    rows, groups = field_ref.shape[:2]
    greet(sizes)
    sources, slots, fills = [], [], []
    first = 0
    for step, count in zip(NEIGHBOURS, pieces(rows, groups)):
        dr, dc = step
        rsel = slice(0, rows) if dr == 0 else (slice(0, HALO) if dr < 0 else slice(rows - HALO, rows))
        slot = halo_ref.at[pl.ds(first, count)]
        if dc == 0:
            sources.append(field_ref.at[rsel])
            slot4 = halo_ref.at[pl.ds(first, count)].reshape(HALO, groups, 8, field_ref.shape[3])
            slots.append(slot4)
        else:
            sources.append(field_ref.at[rsel, 0 if dc < 0 else groups - 1])
            slots.append(slot)

        def fill(first=first, count=count):
            for k in range(0, count, HALO):
                halo_ref[first + k : first + k + HALO] = field_ref[0:HALO, 0]

        fills.append(fill)
        first += count
    finish(swap(sizes, sources, slots, send, recv, fills))


def halo_exchange(sizes, field):
    rows, cols, width = field.shape
    groups = cols // 8
    blocks = sum(pieces(rows, groups))
    return pl.pallas_call(
        functools.partial(halo_kernel, sizes),
        out_shape=jax.ShapeDtypeStruct((blocks, 8, width), BF),
        in_specs=[pl.BlockSpec(memory_space=pltpu.VMEM)],
        out_specs=pl.BlockSpec(memory_space=pltpu.VMEM),
        scratch_shapes=[pltpu.SemaphoreType.DMA((8,)), pltpu.SemaphoreType.DMA((8,))],
        compiler_params=pltpu.CompilerParams(collective_id=0, has_side_effects=True),
        name="halo_exchange",
    )(field.reshape(rows, groups, 8, width))


def layer_kernel(
    sizes, rows, cols,
    field_ref, halo_ref, gains_ref, wq_ref, wk_ref, wv_ref, wo_ref, wu_ref, wd_ref, fg_ref,
    out_ref, left_ref, right_ref,
    q_s, kt_s, va_s, f_s,
):
    tokens, width = field_ref.shape
    head = width // HEADS
    per = 128 // head
    g0 = gains_ref[0:1, :]
    g1 = gains_ref[1:2, :]
    fg = fg_ref[...]
    lane = lax.broadcasted_iota(jnp.int32, (1, 128), 1) // head

    def keep(h, start, ok):
        k = jnp.dot(h, wk_ref[...], preferred_element_type=F32)
        kt_s[:, start : start + h.shape[0]] = k.T.astype(BF)
        v = jnp.dot(h, wv_ref[...], preferred_element_type=F32)
        for e in range(HEADS):
            half = e // per
            part = jnp.where(lane == e % per, v[:, half * 128 : half * 128 + 128], 1.0)
            if ok is not None:
                part = part * ok
            va_s[e, start : start + h.shape[0], :] = part.astype(BF)

    scale = head**-0.5 * 1.4426950408889634
    for start in range(0, tokens, 256):
        h = rms(field_ref[start : start + 256, :].astype(F32), g0).astype(BF)
        q = jnp.dot(h, wq_ref[...], preferred_element_type=F32) * scale
        q_s[start : start + 256, :] = q.astype(BF)
        keep(h, start, None)
    first = 0
    groups = cols // 8
    marks = []
    for step, count in zip(NEIGHBOURS, pieces(rows, groups)):
        ok = there(step, sizes)[0].astype(F32)
        marks.append((first * 8, count * 8, ok))
        first += count
    total = first * 8
    for start in range(0, total, 128):
        h = rms(halo_ref[start : start + 128, :].astype(F32), g0).astype(BF)
        row = lax.broadcasted_iota(jnp.int32, (128, 1), 0) + start
        ok = jnp.zeros((128, 1), F32)
        for at, count, flag in marks:
            if at < start + 128 and at + count > start:
                ok = jnp.where((row >= at) & (row < at + count), flag, ok)
        keep(h, tokens + start, ok)

    def body(index, carry):
        at = pl.ds(pl.multiple_of(index * CHUNK, CHUNK), CHUNK)
        halves = []
        for half in range(width // 128):
            qh = q_s[at, half * 128 : half * 128 + 128]
            ctx = jnp.zeros((CHUNK, 128), F32)
            for e in range(per):
                qm = jnp.where(lane == e, qh, jnp.zeros_like(qh))
                s = jnp.dot(qm, kt_s[half * 128 : half * 128 + 128, :], preferred_element_type=F32)
                m = jnp.max(s, axis=-1, keepdims=True)
                p = jnp.exp2(s - m).astype(BF)
                o = jnp.dot(p, va_s[half * per + e], preferred_element_type=F32)
                ctx = jnp.where(lane == e, o / pltpu.roll(o, head, 1), ctx)
            halves.append(ctx.astype(BF))
        ctx = jnp.concatenate(halves, axis=1)
        x = field_ref[at, :].astype(F32) + jnp.dot(ctx, wo_ref[...], preferred_element_type=F32)
        h = rms(x, g1).astype(BF)
        u = jax.nn.gelu(jnp.dot(h, wu_ref[...], preferred_element_type=F32)).astype(BF)
        x = x + jnp.dot(u, wd_ref[...], preferred_element_type=F32)
        f = rms(x, fg)
        out_ref[at, :] = f.astype(BF)
        for half in range(width // 128):
            f_s[half, at, :] = f[:, half * 128 : half * 128 + 128]
        return carry

    lax.fori_loop(0, tokens // CHUNK, body, 0)
    for half in range(width // 128):
        sl = slice(half * 128, half * 128 + 128)
        left_ref[:, sl] = f_s[half, pl.ds(0, rows, stride=cols), :].astype(BF)
        right_ref[:, sl] = f_s[half, pl.ds(cols - 1, rows, stride=cols), :].astype(BF)


def layer(sizes, rows, cols, field, halo, gains, wq, wk, wv, wo, wu, wd, fg):
    tokens, width = field.shape
    keys = tokens + halo.shape[0]
    vm = pl.BlockSpec(memory_space=pltpu.VMEM)
    return pl.pallas_call(
        functools.partial(layer_kernel, sizes, rows, cols),
        out_shape=(
            jax.ShapeDtypeStruct((tokens, width), BF),
            jax.ShapeDtypeStruct((rows, width), BF),
            jax.ShapeDtypeStruct((rows, width), BF),
        ),
        in_specs=[vm] * 10,
        out_specs=(vm, vm, vm),
        scratch_shapes=[
            pltpu.VMEM((tokens, width), BF),
            pltpu.VMEM((width, keys), BF),
            pltpu.VMEM((HEADS, keys, 128), BF),
            pltpu.VMEM((width // 128, tokens, 128), F32),
        ],
        compiler_params=pltpu.CompilerParams(vmem_limit_bytes=VMEM_LIMIT),
        name="layer",
    )(field, halo, gains, wq, wk, wv, wo, wu, wd, fg)


def conv_kernel(
    sizes,
    final_ref, left_ref, right_ref, weight_ref,
    image_ref,
    row_h, col_h, cor_h, fb_s, wp_s, up_s, send, recv,
):
    rows, cols, width = final_ref.shape
    tokens = rows * cols
    outs = weight_ref.shape[1]
    greet(sizes)
    slots = [row_h.at[0], row_h.at[1], col_h.at[0], col_h.at[1]] + [cor_h.at[n] for n in range(4)]
    sources = [
        final_ref.at[0], final_ref.at[rows - 1], left_ref, right_ref,
        left_ref.at[pl.ds(0, 8)], right_ref.at[pl.ds(0, 8)],
        left_ref.at[pl.ds(rows - 8, 8)], right_ref.at[pl.ds(rows - 8, 8)],
    ]

    def filler(slot):
        def fill():
            slot[...] = jnp.zeros(slot.shape, BF)
        return fill

    copies = swap(sizes, sources, slots, send, recv, [filler(s) for s in slots])
    old = lax.broadcasted_iota(jnp.int32, (outs, outs), 0)
    new = lax.broadcasted_iota(jnp.int32, (outs, outs), 1)
    want = (new % (outs // SHUF)) * SHUF + new // (outs // SHUF)
    perm = jnp.where(old == want, 1.0, 0.0).astype(BF)
    for tap in range(9):
        sl = slice(tap * width, (tap + 1) * width)
        wp_s[sl, :] = jnp.dot(weight_ref[sl, :], perm, preferred_element_type=F32).astype(BF)
    finish(copies)

    col = lax.broadcasted_iota(jnp.int32, (1, cols, 1), 1)

    def spread(first, count, x, before, after):
        flat = x.reshape(count * cols, width)
        low = pltpu.roll(flat, 1, 0).reshape(count, cols, width)
        high = pltpu.roll(flat, count * cols - 1, 0).reshape(count, cols, width)
        fb_s[1, first : first + count] = x.astype(BF)
        fb_s[0, first : first + count] = jnp.where(col == 0, before, low).astype(BF)
        fb_s[2, first : first + count] = jnp.where(col == cols - 1, after, high).astype(BF)

    for r in range(0, rows, 8):
        before = col_h[0, r : r + 8, :].astype(F32)[:, None, :]
        after = col_h[1, r : r + 8, :].astype(F32)[:, None, :]
        spread(1 + r, 8, final_ref[r : r + 8].astype(F32), before, after)
    for side, at, pick in ((0, 0, 7), (1, rows + 1, 0)):
        before = cor_h[2 * side].astype(F32)[pick : pick + 1][:, None, :]
        after = cor_h[2 * side + 1].astype(F32)[pick : pick + 1][:, None, :]
        spread(at, 1, row_h[side].astype(F32)[None], before, after)

    step = 8
    quarter = outs // SHUF
    for r in range(0, rows, step):
        acc = jnp.zeros((step * cols, outs), F32)
        for a in range(3):
            for b in range(3):
                tap = a * 3 + b
                acc = acc + jnp.dot(
                    fb_s[b, r + a : r + a + step].reshape(step * cols, width),
                    wp_s[tap * width : (tap + 1) * width, :],
                    preferred_element_type=F32,
                )
        for k in range(step):
            part = acc[k * cols : (k + 1) * cols]
            slot = k % 2
            for j in range(SHUF):
                pair = j * quarter // 128
                up_s[slot, pl.ds(j, cols, stride=SHUF), :] = part[:, pair * 128 : pair * 128 + 128]
            t = up_s[slot].T
            lanes = lax.broadcasted_iota(jnp.int32, (1, cols * SHUF), 1)
            t = jnp.where(lanes % 2 == 0, t[:quarter], t[quarter : 2 * quarter])
            for c in range(quarter // SHUF):
                image_ref[c, (r + k) * SHUF : (r + k + 1) * SHUF, :] = t[c * SHUF : (c + 1) * SHUF]


def conv_image(sizes, final, left, right, weight):
    rows, cols, width = final.shape
    outs = weight.shape[1]
    vm = pl.BlockSpec(memory_space=pltpu.VMEM)
    return pl.pallas_call(
        functools.partial(conv_kernel, sizes),
        out_shape=jax.ShapeDtypeStruct((outs // SHUF**2, rows * SHUF, cols * SHUF), F32),
        in_specs=[vm] * 4,
        out_specs=vm,
        scratch_shapes=[
            pltpu.VMEM((2, cols, width), BF),
            pltpu.VMEM((2, rows, width), BF),
            pltpu.VMEM((4, 8, width), BF),
            pltpu.VMEM((3, rows + 2, cols, width), BF),
            pltpu.VMEM(weight.shape, BF),
            pltpu.VMEM((2, cols * SHUF, 128), F32),
            pltpu.SemaphoreType.DMA((8,)),
            pltpu.SemaphoreType.DMA((8,)),
        ],
        compiler_params=pltpu.CompilerParams(
            collective_id=1, has_side_effects=True, vmem_limit_bytes=VMEM_LIMIT
        ),
        name="conv_image",
    )(final, left, right, weight)


def local(sizes, field, gains, w_query, w_key, w_value, w_out, w_up, w_down, final_gain, conv_weight):
    rows, cols, width = field.shape
    halo = halo_exchange(sizes, field).reshape(-1, width)
    final, left, right = layer(
        sizes, rows, cols, field.reshape(-1, width), halo, gains[0], w_query[0], w_key[0],
        w_value[0], w_out[0], w_up[0], w_down[0], final_gain[None, :],
    )
    weight = conv_weight.reshape(-1, conv_weight.shape[3])
    return conv_image(sizes, final.reshape(rows, cols, width), left, right, weight)


def solution(mesh):
    sizes = (mesh.shape["row"], mesh.shape["col"])
    return jax.shard_map(
        functools.partial(local, sizes),
        mesh=mesh,
        in_specs=(P("row", "col", None), P(), P(), P(), P(), P(), P(), P(), P(), P()),
        out_specs=P(None, "row", "col"),
        check_vma=False,
    )
```

```python
import functools

import jax
import jax.numpy as jnp
from jax import lax
from jax.experimental import pallas as pl
from jax.experimental.pallas import tpu as pltpu
from jax.sharding import PartitionSpec as P

HEADS = 8
HALO = 8
SHUF = 4
CHUNK = 256
VMEM_LIMIT = 56 * 1024 * 1024
BF = jnp.bfloat16
F32 = jnp.float32
NEIGHBOURS = ((-1, 0), (1, 0), (0, -1), (0, 1), (-1, -1), (-1, 1), (1, -1), (1, 1))


def rms(values, gain):
    return values * lax.rsqrt(jnp.mean(values * values, axis=-1, keepdims=True) + 1e-06) * gain


def there(step, sizes):
    row, col = lax.axis_index("row"), lax.axis_index("col")
    nrow, ncol = row + step[0], col + step[1]
    ok = (nrow >= 0) & (nrow < sizes[0]) & (ncol >= 0) & (ncol < sizes[1])
    return ok, nrow, ncol


def greet(sizes):
    barrier = pltpu.get_barrier_semaphore()
    for step in NEIGHBOURS:
        ok, nrow, ncol = there(step, sizes)

        @pl.when(ok)
        def _():
            pl.semaphore_signal(
                barrier, inc=1, device_id=(nrow, ncol), device_id_type=pl.DeviceIdType.MESH
            )

    peers = jnp.int32(0)
    for step in NEIGHBOURS:
        peers = peers + there(step, sizes)[0].astype(jnp.int32)
    pl.semaphore_wait(barrier, peers)


def swap(sizes, sources, slots, send, recv, fills):
    copies = []
    for n, step in enumerate(NEIGHBOURS):
        ok, nrow, ncol = there(step, sizes)
        back = NEIGHBOURS.index((-step[0], -step[1]))
        copy = pltpu.make_async_remote_copy(
            src_ref=sources[n],
            dst_ref=slots[back],
            send_sem=send.at[n],
            recv_sem=recv.at[back],
            device_id=(nrow, ncol),
            device_id_type=pl.DeviceIdType.MESH,
        )
        arrival = pltpu.make_async_remote_copy(
            src_ref=slots[n],
            dst_ref=slots[n],
            send_sem=send.at[n],
            recv_sem=recv.at[n],
            device_id=(nrow, ncol),
            device_id_type=pl.DeviceIdType.MESH,
        )
        copies.append((ok, copy, arrival))
        pl.when(ok)(copy.start)
        pl.when(jnp.logical_not(ok))(fills[n])
    return copies


def finish(copies):
    for ok, copy, arrival in copies:
        pl.when(ok)(arrival.wait_recv)
    for ok, copy, _ in copies:
        pl.when(ok)(copy.wait_send)


def pieces(rows, groups):
    return [HALO * groups] * 2 + [rows] * 2 + [HALO] * 4


def halo_start(sizes, field_ref, halo_ref, send, recv):
    rows, groups = field_ref.shape[:2]
    sources, slots, fills = [], [], []
    first = 0
    for step, count in zip(NEIGHBOURS, pieces(rows, groups)):
        dr, dc = step
        rsel = slice(0, rows) if dr == 0 else (slice(0, HALO) if dr < 0 else slice(rows - HALO, rows))
        slot = halo_ref.at[pl.ds(first, count)]
        if dc == 0:
            sources.append(field_ref.at[rsel])
            slots.append(slot.reshape(HALO, groups, 8, field_ref.shape[3]))
        else:
            sources.append(field_ref.at[rsel, 0 if dc < 0 else groups - 1])
            slots.append(slot)

        def fill(first=first, count=count):
            for k in range(0, count, HALO):
                halo_ref[first + k : first + k + HALO] = field_ref[0:HALO, 0]

        fills.append(fill)
        first += count
    return swap(sizes, sources, slots, send, recv, fills)


def layer_kernel(
    sizes,
    field_ref, gains_ref, wq_ref, wk_ref, wv_ref, wo_hbm, wu_hbm, wd_hbm, fg_ref,
    out_ref, row_h, col_h, cor_h,
    halo_ref, q_s, kt_s, va_s, f_s, o_s, m_s, left_s, right_s, wo_ref, wu_ref, wd_ref,
    send, recv, send2, recv2, wsem,
):
    rows, groups = field_ref.shape[:2]
    cols = groups * 8
    tokens, width = q_s.shape
    head = width // HEADS
    per = 128 // head
    loads = [
        pltpu.make_async_copy(src, dst, wsem.at[n])
        for n, (src, dst) in enumerate(((wo_hbm, wo_ref), (wu_hbm, wu_ref), (wd_hbm, wd_ref)))
    ]
    for load in loads:
        load.start()
    greet(sizes)
    copies = halo_start(sizes, field_ref, halo_ref, send, recv)

    g0 = gains_ref[0:1, :]
    g1 = gains_ref[1:2, :]
    fg = fg_ref[...]
    lane = lax.broadcasted_iota(jnp.int32, (1, 128), 1) // head

    def keep(h, start, ok):
        k = jnp.dot(h, wk_ref[...], preferred_element_type=F32)
        kt_s[:, start : start + h.shape[0]] = k.T.astype(BF)
        v = jnp.dot(h, wv_ref[...], preferred_element_type=F32)
        for e in range(HEADS):
            half = e // per
            part = jnp.where(lane == e % per, v[:, half * 128 : half * 128 + 128], 1.0)
            if ok is not None:
                part = part * ok
            va_s[e, start : start + h.shape[0], :] = part.astype(BF)

    scale = head**-0.5 * 1.4426950408889634
    span = CHUNK // cols
    for start in range(0, tokens, CHUNK):
        at = start // cols
        h = rms(field_ref[at : at + span].astype(F32).reshape(CHUNK, width), g0).astype(BF)
        q = jnp.dot(h, wq_ref[...], preferred_element_type=F32) * scale
        q_s[start : start + CHUNK, :] = q.astype(BF)
        keep(h, start, None)

    def head_part(at, half, e, first, count):
        qh = q_s[at, half * 128 : half * 128 + 128]
        qm = jnp.where(lane == e, qh, jnp.zeros_like(qh))
        keys = slice(first, first + count)
        s = jnp.dot(qm, kt_s[half * 128 : half * 128 + 128, keys], preferred_element_type=F32)
        m = jnp.max(s, axis=-1, keepdims=True)
        p = jnp.exp2((s - m).astype(BF))
        return m, jnp.dot(p, va_s[half * per + e, keys, :], preferred_element_type=F32)

    def own(index, carry):
        at = pl.ds(pl.multiple_of(index * CHUNK, CHUNK), CHUNK)
        for half in range(width // 128):
            for e in range(per):
                m, o = head_part(at, half, e, 0, tokens)
                o_s[half * per + e, at, :] = o
                m_s[half * per + e, at, :] = jnp.broadcast_to(m, o.shape)
        return carry

    lax.fori_loop(0, tokens // CHUNK, own, 0)
    finish(copies)

    first = 0
    marks = []
    for step, count in zip(NEIGHBOURS, pieces(rows, groups)):
        ok = there(step, sizes)[0].astype(F32)
        marks.append((first * 8, count * 8, ok))
        first += count
    total = first * 8
    for start in range(0, total, 128):
        raw = halo_ref[start // 8 : start // 8 + 16].astype(F32).reshape(128, width)
        h = rms(raw, g0).astype(BF)
        row = lax.broadcasted_iota(jnp.int32, (128, 1), 0) + start
        ok = jnp.zeros((128, 1), F32)
        for at, count, flag in marks:
            if at < start + 128 and at + count > start:
                ok = jnp.where((row >= at) & (row < at + count), flag, ok)
        keep(h, tokens + start, ok)
    for load in loads:
        load.wait()

    def body(index, carry):
        at = pl.ds(pl.multiple_of(index * CHUNK, CHUNK), CHUNK)
        halves = []
        for half in range(width // 128):
            ctx = jnp.zeros((CHUNK, 128), F32)
            for e in range(per):
                m, o = head_part(at, half, e, tokens, total)
                old = m_s[half * per + e, at, :]
                top = jnp.maximum(old, m)
                o = o * jnp.exp2(m - top) + o_s[half * per + e, at, :] * jnp.exp2(old - top)
                ctx = jnp.where(lane == e, o / pltpu.roll(o, head, 1), ctx)
            halves.append(ctx.astype(BF))
        ctx = jnp.concatenate(halves, axis=1)
        x = field_ref[pl.ds(index * span, span)].astype(F32).reshape(CHUNK, width)
        x = x + jnp.dot(ctx, wo_ref[...], preferred_element_type=F32)
        h = rms(x, g1).astype(BF)
        u = jax.nn.gelu(jnp.dot(h, wu_ref[...], preferred_element_type=F32)).astype(BF)
        x = x + jnp.dot(u, wd_ref[...], preferred_element_type=F32)
        f = rms(x, fg)
        out_ref[pl.ds(index * span, span)] = f.reshape(span, cols, width).astype(BF)
        for half in range(width // 128):
            f_s[half, at, :] = f[:, half * 128 : half * 128 + 128]
        return carry

    lax.fori_loop(0, tokens // CHUNK, body, 0)
    for half in range(width // 128):
        sl = slice(half * 128, half * 128 + 128)
        left_s[:, sl] = f_s[half, pl.ds(0, rows, stride=cols), :].astype(BF)
        right_s[:, sl] = f_s[half, pl.ds(cols - 1, rows, stride=cols), :].astype(BF)
    slots = [row_h.at[0], row_h.at[1], col_h.at[0], col_h.at[1]] + [cor_h.at[n] for n in range(4)]
    sources = [
        out_ref.at[0], out_ref.at[rows - 1], left_s, right_s,
        left_s.at[pl.ds(0, 8)], right_s.at[pl.ds(0, 8)],
        left_s.at[pl.ds(rows - 8, 8)], right_s.at[pl.ds(rows - 8, 8)],
    ]

    def filler(slot):
        def fill():
            slot[...] = jnp.zeros(slot.shape, BF)
        return fill

    finish(swap(sizes, sources, slots, send2, recv2, [filler(s) for s in slots]))


def layer(sizes, field, gains, wq, wk, wv, wo, wu, wd, fg):
    rows, cols, width = field.shape
    groups = cols // 8
    tokens = rows * cols
    blocks = sum(pieces(rows, groups))
    keys = tokens + blocks * 8
    vm = pl.BlockSpec(memory_space=pltpu.VMEM)
    hbm = pl.BlockSpec(memory_space=pl.ANY)
    eight = pltpu.SemaphoreType.DMA((8,))
    return pl.pallas_call(
        functools.partial(layer_kernel, sizes),
        out_shape=(
            jax.ShapeDtypeStruct((rows, cols, width), BF),
            jax.ShapeDtypeStruct((2, cols, width), BF),
            jax.ShapeDtypeStruct((2, rows, width), BF),
            jax.ShapeDtypeStruct((4, 8, width), BF),
        ),
        in_specs=[vm] * 5 + [hbm] * 3 + [vm],
        out_specs=(vm,) * 4,
        scratch_shapes=[
            pltpu.VMEM((blocks, 8, width), BF),
            pltpu.VMEM((tokens, width), BF),
            pltpu.VMEM((width, keys), BF),
            pltpu.VMEM((HEADS, keys, 128), BF),
            pltpu.VMEM((width // 128, tokens, 128), F32),
            pltpu.VMEM((HEADS, tokens, 128), F32),
            pltpu.VMEM((HEADS, tokens, 128), F32),
            pltpu.VMEM((rows, width), BF),
            pltpu.VMEM((rows, width), BF),
            pltpu.VMEM(wo.shape, BF),
            pltpu.VMEM(wu.shape, BF),
            pltpu.VMEM(wd.shape, BF),
            eight, eight, eight, eight,
            pltpu.SemaphoreType.DMA((3,)),
        ],
        compiler_params=pltpu.CompilerParams(
            collective_id=0, has_side_effects=True, vmem_limit_bytes=VMEM_LIMIT
        ),
        name="layer",
    )(field.reshape(rows, groups, 8, width), gains, wq, wk, wv, wo, wu, wd, fg)


def conv_kernel(final_ref, row_h, col_h, cor_h, weight_ref, image_ref, fb_s, wp_s, up_s):
    rows, cols, width = final_ref.shape
    tokens = rows * cols
    outs = weight_ref.shape[1]
    old = lax.broadcasted_iota(jnp.int32, (outs, outs), 0)
    new = lax.broadcasted_iota(jnp.int32, (outs, outs), 1)
    want = (new % (outs // SHUF)) * SHUF + new // (outs // SHUF)
    perm = jnp.where(old == want, 1.0, 0.0).astype(BF)
    for tap in range(9):
        sl = slice(tap * width, (tap + 1) * width)
        wp_s[sl, :] = jnp.dot(weight_ref[sl, :], perm, preferred_element_type=F32).astype(BF)
    col = lax.broadcasted_iota(jnp.int32, (1, cols, 1), 1)

    def spread(first, count, x, before, after):
        flat = x.reshape(count * cols, width)
        low = pltpu.roll(flat, 1, 0).reshape(count, cols, width)
        high = pltpu.roll(flat, count * cols - 1, 0).reshape(count, cols, width)
        fb_s[1, first : first + count] = x.astype(BF)
        fb_s[0, first : first + count] = jnp.where(col == 0, before, low).astype(BF)
        fb_s[2, first : first + count] = jnp.where(col == cols - 1, after, high).astype(BF)

    for r in range(0, rows, 8):
        before = col_h[0, r : r + 8, :].astype(F32)[:, None, :]
        after = col_h[1, r : r + 8, :].astype(F32)[:, None, :]
        spread(1 + r, 8, final_ref[r : r + 8].astype(F32), before, after)
    for side, at, pick in ((0, 0, 7), (1, rows + 1, 0)):
        before = cor_h[2 * side].astype(F32)[pick : pick + 1][:, None, :]
        after = cor_h[2 * side + 1].astype(F32)[pick : pick + 1][:, None, :]
        spread(at, 1, row_h[side].astype(F32)[None], before, after)

    step = 8
    quarter = outs // SHUF
    for r in range(0, rows, step):
        acc = jnp.zeros((step * cols, outs), F32)
        for a in range(3):
            for b in range(3):
                tap = a * 3 + b
                acc = acc + jnp.dot(
                    fb_s[b, r + a : r + a + step].reshape(step * cols, width),
                    wp_s[tap * width : (tap + 1) * width, :],
                    preferred_element_type=F32,
                )
        for k in range(step):
            part = acc[k * cols : (k + 1) * cols]
            slot = k % 2
            for j in range(SHUF):
                pair = j * quarter // 128
                up_s[slot, pl.ds(j, cols, stride=SHUF), :] = part[:, pair * 128 : pair * 128 + 128]
            t = up_s[slot].T
            lanes = lax.broadcasted_iota(jnp.int32, (1, cols * SHUF), 1)
            t = jnp.where(lanes % 2 == 0, t[:quarter], t[quarter : 2 * quarter])
            for c in range(quarter // SHUF):
                image_ref[c, (r + k) * SHUF : (r + k + 1) * SHUF, :] = t[c * SHUF : (c + 1) * SHUF]


def conv_image(final, row, col, corner, weight):
    rows, cols, width = final.shape
    outs = weight.shape[1]
    vm = pl.BlockSpec(memory_space=pltpu.VMEM)
    return pl.pallas_call(
        conv_kernel,
        out_shape=jax.ShapeDtypeStruct((outs // SHUF**2, rows * SHUF, cols * SHUF), F32),
        in_specs=[vm] * 5,
        out_specs=vm,
        scratch_shapes=[
            pltpu.VMEM((3, rows + 2, cols, width), BF),
            pltpu.VMEM(weight.shape, BF),
            pltpu.VMEM((2, cols * SHUF, 128), F32),
        ],
        compiler_params=pltpu.CompilerParams(vmem_limit_bytes=VMEM_LIMIT),
        name="conv_image",
    )(final, row, col, corner, weight)


def local(sizes, field, gains, w_query, w_key, w_value, w_out, w_up, w_down, final_gain, conv_weight):
    final, row, col, corner = layer(
        sizes, field, gains[0], w_query[0], w_key[0], w_value[0], w_out[0], w_up[0], w_down[0],
        final_gain[None, :],
    )
    weight = conv_weight.reshape(-1, conv_weight.shape[3])
    return conv_image(final, row, col, corner, weight)


def solution(mesh):
    sizes = (mesh.shape["row"], mesh.shape["col"])
    return jax.shard_map(
        functools.partial(local, sizes),
        mesh=mesh,
        in_specs=(P("row", "col", None), P(), P(), P(), P(), P(), P(), P(), P(), P()),
        out_specs=P(None, "row", "col"),
        check_vma=False,
    )
```
